32 devices in a mesh: row: 4 (over x, core), col: 4 (over z), layer: 2 (over y).
Axes of the slice: x: 2, y: 2, z: 4, core: 2. Of those that a mesh axis runs over, the one named last changes fastest.
Arguments:
- left_factor: float32 [6144, 8192], P('row', 'col'), may hold values from -6 to 6
- right_factor: float32 [8192, 6144], P('row', 'col'), may hold values from -0.0625 to 0.0625
Outputs:
- product: float32 [6144, 6144], P(('row', 'layer'), 'col')
The draws below stay inside these ranges and needn't reach their ends.
All inputs are finite; a program needn't handle non-finite values.
Results may differ from the reference program's by a relative error of at most 0.000073.
Values sent between devices are 32-bit elements; how exact they have to be, the bound alone decides.
A program may use at most 192 MiB of HBM per device.

```python
import jax
import jax.numpy as jnp
from jax import lax

K = 8192
M = 6144
NC = 6144


def spiked(drawn, stream_key, source, target, blocks, factor):
    def block_of(dim):
        return (jnp.arange(drawn.shape[dim]) // (drawn.shape[dim] // blocks)).reshape((-1,) + (1,) * (drawn.ndim - 1 - dim))

    one_side = jax.random.permutation(stream_key, blocks)[block_of(target)]
    second = (block_of(target) + blocks // 2) % blocks
    return jnp.where((block_of(source) == one_side) | (block_of(source) == second), factor * drawn, drawn)


def block_scale(rng, dims, split, least, top_value):
    gain = 1.0
    for position, shards_of in split:
        draws = jax.random.uniform(jax.random.fold_in(jax.random.fold_in(rng, 6), position), (shards_of,), jnp.float32, least / len(split), top_value / len(split))
        gain = gain * jnp.repeat(jnp.exp(draws), dims[position] // shards_of).reshape((-1,) + (1,) * (len(dims) - 1 - position))
    return gain


def gaussian(key, dims, scale, reach, pieces=(), held_as=jnp.bfloat16):
    drawn = scale * jax.random.normal(key, dims, jnp.float32)
    if pieces:
        drawn = drawn * block_scale(key, dims, pieces, -0.22, 0.18)
    return jnp.clip(drawn, -reach, reach).astype(held_as)


def noise_with(key, dims, spread, most, cuts, heavy, dtype=jnp.bfloat16):
    drawn = spread * jax.random.normal(key, dims, jnp.float32)
    if cuts:
        drawn = drawn * block_scale(key, dims, cuts, -0.22, 0.18)
    return jnp.clip(spiked(drawn, jax.random.fold_in(key, 3), *heavy), -most, most).astype(dtype)


def setup_inputs(seed: int = 0) -> dict:
    seeds = jax.random.split(jax.random.key(seed), 3)
    return {
        "left_factor": noise_with(seeds[0], (M, K), 1.0, 6.0, ((0, 4), (1, 4)), (1, 0, 4, 2.0), jnp.float32),
        "right_factor": gaussian(seeds[1], (K, NC), K ** -0.5, 0.0625, ((0, 4), (1, 4)), jnp.float32),
    }


def reference(left_factor, right_factor):
    return jnp.dot(left_factor, right_factor, precision=lax.Precision.HIGHEST, preferred_element_type=jnp.float32)
```

```python
import jax
import jax.numpy as jnp
from jax import lax
from jax.sharding import PartitionSpec as P

CHUNKS = 2


def product(left, right):
    return jnp.dot(
        left,
        right,
        precision=lax.Precision.HIGH,
        preferred_element_type=jnp.float32,
    )


def gathered(left_factor, right_factor):
    layers = lax.axis_size("layer")
    rows = left_factor.shape[0] // layers
    left = lax.dynamic_slice_in_dim(left_factor, lax.axis_index("layer") * rows, rows, 0)
    left = lax.all_gather(left, "col", axis=1, tiled=True)
    right = lax.all_gather(right_factor, "row", axis=0, tiled=True)
    return product(left, right)


def line(left_factor, right_factor):
    row, col, layer = (lax.axis_index(name) for name in ("row", "col", "layer"))
    rows = left_factor.shape[0] // 2
    depth = left_factor.shape[1]
    piece = depth // CHUNKS
    mine = lax.dynamic_slice_in_dim(left_factor, layer * rows, rows, 0)
    up = [(0, 1), (1, 2), (2, 3)]
    down = [(1, 0), (2, 1), (3, 2)]
    across = [(0, 2), (2, 0), (1, 3), (3, 1)]
    mate = [(0, 1), (1, 0), (2, 3), (3, 2)]
    swap = [(0, 1), (1, 0)]

    own = [mine[:, c * piece : (c + 1) * piece] for c in range(CHUNKS)]
    rising, falling = [own], [own]
    for step in range(3):
        edge = up if step == 0 else up[step:]
        back = down if step == 0 else down[: 3 - step]
        rising.append([lax.ppermute(part, "col", edge) for part in rising[-1]])
        falling.append([lax.ppermute(part, "col", back) for part in falling[-1]])

    half = depth // 2
    cut = half // CHUNKS
    low, high = [], []
    for c in range(CHUNKS):
        sent = lax.dynamic_slice_in_dim(right_factor, layer * half + c * cut, cut, 0)
        here = lax.ppermute(sent, "row", across)
        there = lax.ppermute(here, "layer", swap)
        low.append(jnp.where(layer == 0, here, there))
        high.append(jnp.where(layer == 0, there, here))
    beside = lax.ppermute(right_factor, "row", mate)
    far = low + high
    far_beside = [lax.ppermute(part, "row", mate) for part in far]
    right = jnp.concatenate([right_factor, beside] + far + far_beside, 0)

    def term(left, block, c):
        start = jnp.bitwise_xor(row, block) * depth + c * piece
        return product(left, lax.dynamic_slice_in_dim(right, start, piece, 0))

    near = col <= 1
    total = 0.0
    for c in range(CHUNKS):
        total += term(own[c], col, c)
    for c in range(CHUNKS):
        total += term(jnp.where(near, falling[1][c], rising[1][c]), jnp.where(near, col + 1, col - 1), c)
    for c in range(CHUNKS):
        total += term(jnp.where(near, falling[2][c], rising[2][c]), jnp.where(near, col + 2, col - 2), c)
    for c in range(CHUNKS):
        last = jnp.where(near, rising[1][c], falling[1][c])
        last = jnp.where(col == 0, falling[3][c], jnp.where(col == 3, rising[3][c], last))
        block = jnp.where(col == 0, 3, jnp.where(col == 3, 0, jnp.where(near, col - 1, col + 1)))
        total += term(last, block, c)
    return total


def solution(mesh):
    placed = (P("row", "col"), P("row", "col"))
    fits = (mesh.shape["row"], mesh.shape["col"], mesh.shape["layer"]) == (4, 4, 2)
    return jax.shard_map(
        line if fits else gathered,
        mesh=mesh,
        in_specs=placed,
        out_specs=P(("row", "layer"), "col"),
        check_vma=False,
    )
```
